256 devices in a mesh: rows: 64 (over z, y, core), cols: 4 (over x).
Axes of the slice: x: 4, y: 4, z: 8, core: 2. Of those that a mesh axis runs over, the one named last changes fastest.
Arguments:
- gradients: float32 [256, 128, 4096], P(None, 'rows', 'cols'), may hold values from -6 to 6
- momentum: float32 [256, 128, 4096], P(None, 'rows', 'cols'), may hold values from -6 to 6
- weights: float32 [256, 128, 4096], P(None, 'rows', 'cols'), may hold values from -0.1875 to 0.1875
Outputs:
- new_weights: float32 [256, 128, 4096], P(None, 'rows', 'cols')
- new_momentum: float32 [256, 128, 4096], P(None, 'rows', 'cols')
The draws below stay inside these ranges and needn't reach their ends.
All inputs are finite; a program needn't handle non-finite values.
Results may differ from the reference program's by a relative error of at most 0.0003.
Values sent between devices are 32-bit elements.
No kernel may reach another device: no remote copies, remote signals or barrier semaphores. Data moves between devices by JAX's collectives and lax.ppermute only.
A program may use at most 64 MiB of HBM per device.

```python
import jax
import jax.numpy as jnp
from jax import lax

SIDE = 128
WIDE = 4096
MATS = 256
ITERS = 4


def level_of(stream_key, dims, pieces, least, largest):
    def one(dim, blocks):
        steps = jax.random.uniform(jax.random.fold_in(jax.random.fold_in(stream_key, 6), dim), (blocks,), jnp.float32, least / len(pieces), largest / len(pieces))
        return jnp.repeat(jnp.exp(steps), dims[dim] // blocks).reshape((-1,) + (1,) * (len(dims) - dim - 1))

    gain = one(*pieces[0])
    for cut in pieces[1:]:
        gain = gain * one(*cut)
    return gain


def noise(stream_key, extent, scale, limit, cuts=(), kind=jnp.bfloat16):
    result = scale * jax.random.normal(stream_key, extent, jnp.float32)
    if cuts:
        result = result * level_of(stream_key, extent, cuts, -0.22, 0.18)
    return jnp.clip(result, -limit, limit).astype(kind)


def setup_inputs(seed: int = 0) -> dict:
    streams_of = jax.random.split(jax.random.key(seed), 4)
    return {
        "gradients": noise(streams_of[0], (MATS, SIDE, WIDE), 1.0, 6.0, ((1, 64), (2, 4)), jnp.float32),
        "momentum": noise(streams_of[1], (MATS, SIDE, WIDE), 1.0, 6.0, ((1, 64), (2, 4)), jnp.float32),
        "weights": noise(streams_of[2], (MATS, SIDE, WIDE), 0.03, 0.1875, ((1, 64), (2, 4)), jnp.float32),
    }


hold_rate = 0.8
learn_rate = 0.8
decay_rate = 0.1

def reference(gradients, momentum, weights):
    new_momentum = hold_rate * momentum + gradients

    def orthogonal_one(stack):
        iterate = stack[None]
        iterate = iterate * lax.rsqrt(lax.optimization_barrier(jnp.sum(iterate * iterate, axis=(1, 2), keepdims=True)) + 1e-06)
        for step in range(ITERS):
            gram = jnp.einsum('mik,mjk->mij', iterate, iterate, precision=lax.Precision.HIGHEST)
            mixed = -4.775 * gram + 2.0315 * jnp.einsum('mij,mjk->mik', gram, gram, precision=lax.Precision.HIGHEST)
            iterate = 3.4445 * iterate + jnp.einsum('mij,mjk->mik', mixed, iterate, precision=lax.Precision.HIGHEST)
        return iterate[0]
    iterate = lax.map(orthogonal_one, new_momentum)
    new_weights = (1.0 - learn_rate * decay_rate) * weights - learn_rate * iterate
    return (new_weights, new_momentum)
```

```python
import functools

import jax
import jax.numpy as jnp
from jax import lax
from jax.experimental import pallas as pl
from jax.experimental.pallas import tpu as pltpu
from jax.sharding import PartitionSpec as P

ITERS = 4

hold_rate = 0.8
learn_rate = 0.8
decay_rate = 0.1

LANES = 128
SIDE = 128


def flat(x):
    mats, rows, wide = x.shape
    x = x.reshape(mats, rows, wide // LANES, LANES)
    return x.transpose(0, 2, 1, 3).reshape(-1, LANES)


def unflat(x, shape):
    mats, rows, wide = shape
    x = x.reshape(mats, wide // LANES, rows, LANES)
    return x.transpose(0, 2, 1, 3).reshape(shape)


def split(x):
    high = x.astype(jnp.bfloat16)
    return high, (x - high.astype(jnp.float32)).astype(jnp.bfloat16)


def dot(a, b, dims=((1,), (0,))):
    return lax.dot_general(a, b, (dims, ((), ())), preferred_element_type=jnp.float32)


def dot3(a, b):
    ah, al = split(a)
    bh, bl = split(b)
    return dot(ah, bh) + (dot(ah, bl) + dot(al, bh))


def orthogonal(rows_of, x_ref, y_ref, high_ref, low_ref):
    groups = SIDE // rows_of
    step = x_ref.shape[0] // groups
    tiles = step // rows_of
    for k in range(tiles):
        for r in range(rows_of):
            piece = x_ref[pl.ds(k * rows_of + r, groups, stride=step), :]
            high, low = split(piece)
            at = (slice(r * groups, (r + 1) * groups), slice(k * LANES, (k + 1) * LANES))
            high_ref[at] = high
            low_ref[at] = low
    hh = dot(high_ref[...], high_ref[...], ((1,), (1,)))
    hl = dot(high_ref[...], low_ref[...], ((1,), (1,)))
    gram = hh + (hl + hl.T)
    one = (
        lax.broadcasted_iota(jnp.int32, (SIDE, SIDE), 0)
        == lax.broadcasted_iota(jnp.int32, (SIDE, SIDE), 1)
    ).astype(jnp.float32)
    scale = lax.rsqrt(jnp.sum(gram * one, axis=(0, 1), keepdims=True) + 1e-06)
    gram = gram * scale * scale
    total = None
    for step_ in range(ITERS):
        mixed = 3.4445 * one - 4.775 * gram + 2.0315 * dot3(gram, gram)
        total = mixed if total is None else dot3(mixed, total)
        if step_ < ITERS - 1:
            gram = dot3(mixed, dot3(mixed, gram))
    th, tl = split(total * (learn_rate * scale))
    for k in range(tiles):
        at = (slice(None), slice(k * LANES, (k + 1) * LANES))
        y = dot(th, high_ref[at]) + (dot(th, low_ref[at]) + dot(tl, high_ref[at]))
        for r in range(rows_of):
            y_ref[pl.ds(k * rows_of + r, groups, stride=step), :] = y[r * groups : (r + 1) * groups]


def local(gradients, momentum, weights):
    shape = gradients.shape
    new_momentum = hold_rate * flat(momentum) + flat(gradients)
    axes = ("rows", "cols")
    x = lax.all_to_all(new_momentum, axes, split_axis=0, concat_axis=0, tiled=True)
    wide = x.size // SIDE

    y = pl.pallas_call(
        functools.partial(orthogonal, shape[1]),
        out_shape=jax.ShapeDtypeStruct(x.shape, x.dtype),
        in_specs=[pl.BlockSpec(memory_space=pltpu.VMEM)],
        out_specs=pl.BlockSpec(memory_space=pltpu.VMEM),
        scratch_shapes=[pltpu.VMEM((SIDE, wide), jnp.bfloat16), pltpu.VMEM((SIDE, wide), jnp.bfloat16)],
        name="orthogonal",
    )(x)
    y = lax.all_to_all(y, axes, split_axis=0, concat_axis=0, tiled=True)
    new_weights = (1.0 - learn_rate * decay_rate) * flat(weights) - y
    return (unflat(new_weights, shape), unflat(new_momentum, shape))


def solution(mesh):
    placed = P(None, "rows", "cols")
    return jax.shard_map(
        local,
        mesh=mesh,
        in_specs=(placed, placed, placed),
        out_specs=(placed, placed),
        check_vma=False,
    )
```

```python
import functools

import jax
import jax.numpy as jnp
from jax import lax
from jax.experimental import pallas as pl
from jax.experimental.layout import Layout, with_layout_constraint
from jax.experimental.pallas import tpu as pltpu
from jax.sharding import PartitionSpec as P

ITERS = 4

hold_rate = 0.8
learn_rate = 0.8
decay_rate = 0.1

LANES = 128
SIDE = 128
CUTS = 4
PAD = 8
ROWS = 512
LIMIT = 24 << 20


def tiled(x):
    return with_layout_constraint(x, Layout(major_to_minor=(0, 2, 1, 3)))


def flat(x):
    mats, rows, wide = x.shape
    x = tiled(x.reshape(mats, rows, wide // LANES, LANES))
    return x.transpose(0, 2, 1, 3).reshape(-1, LANES)


def unflat(x, shape):
    mats, rows, wide = shape
    x = x.reshape(mats, wide // LANES, rows, LANES).transpose(0, 2, 1, 3)
    return tiled(x).reshape(shape)


def split(x):
    high = x.astype(jnp.bfloat16)
    return high, (x - high.astype(jnp.float32)).astype(jnp.bfloat16)


def dot(a, b, dims=((1,), (0,))):
    return lax.dot_general(a, b, (dims, ((), ())), preferred_element_type=jnp.float32)


def dot3(a, b):
    ah, al = split(a)
    bh, bl = split(b)
    return dot(ah, bh) + (dot(ah, bl) + dot(al, bh))


def blend_kernel(momentum_ref, gradients_ref, kept_ref):
    kept_ref[...] = hold_rate * momentum_ref[...] + gradients_ref[...]


def decay_kernel(weights_ref, step_ref, out_ref):
    out_ref[...] = (1.0 - learn_rate * decay_rate) * weights_ref[...] - step_ref[...]


def rowwise(kernel, name, limit, a, *rest):
    block = pl.BlockSpec((ROWS, LANES), lambda i: (i, 0))
    return pl.pallas_call(
        kernel,
        grid=(a.shape[0] // ROWS,),
        out_shape=jax.ShapeDtypeStruct(a.shape, a.dtype),
        in_specs=[block] * (1 + len(rest)),
        out_specs=block,
        cost_estimate=pl.CostEstimate(flops=2 * a.size, bytes_accessed=12 * a.size, transcendentals=0),
        compiler_params=pltpu.CompilerParams(vmem_limit_bytes=limit),
        name=name,
    )(a, *rest)


def orthogonal(rows_of, x_ref, y_ref, in_ref, out_ref, both_ref, in_sem, out_sem):
    groups = SIDE // rows_of
    step = x_ref.shape[0] // groups
    room = step + PAD
    span = step // CUTS
    tiles = span // rows_of

    def cut(ref, rows, i):
        return ref.reshape(groups, rows, LANES).at[:, pl.ds(i * span, span), :]

    def fetch(i):
        return pltpu.make_async_copy(cut(x_ref, step, i), cut(in_ref, room, i), in_sem.at[i])

    def store(i):
        return pltpu.make_async_copy(cut(out_ref, room, i), cut(y_ref, step, i), out_sem.at[i])

    for i in range(CUTS):
        fetch(i).start()
    grams = jnp.zeros((SIDE, 2 * SIDE), jnp.float32)
    for i in range(CUTS):
        fetch(i).wait()
        for k in range(tiles):
            for r in range(rows_of):
                high, low = split(in_ref[pl.ds(i * span + k * rows_of + r, groups, stride=room), :])
                columns = slice((i * tiles + k) * LANES, (i * tiles + k + 1) * LANES)
                both_ref[r * groups : (r + 1) * groups, columns] = high
                both_ref[SIDE + r * groups : SIDE + (r + 1) * groups, columns] = low
        columns = slice(i * tiles * LANES, (i + 1) * tiles * LANES)
        grams += dot(both_ref[:SIDE, columns], both_ref[:, columns], ((1,), (1,)))
    cross = grams[:, SIDE:]
    gram = grams[:, :SIDE] + (cross + cross.T)
    one = (
        lax.broadcasted_iota(jnp.int32, (SIDE, SIDE), 0)
        == lax.broadcasted_iota(jnp.int32, (SIDE, SIDE), 1)
    ).astype(jnp.float32)
    scale = lax.rsqrt(jnp.sum(gram * one, axis=(0, 1), keepdims=True) + 1e-06)
    gram = gram * scale * scale
    total = None
    for turn in range(ITERS):
        mixed = 3.4445 * one - 4.775 * gram + 2.0315 * dot3(gram, gram)
        total = mixed if total is None else dot3(mixed, total)
        if turn < ITERS - 1:
            gram = dot3(mixed, dot3(mixed, gram))
    th, tl = split(total * (learn_rate * scale))
    twice = jnp.concatenate([th, th], axis=1)
    for i in range(CUTS):
        columns = slice(i * tiles * LANES, (i + 1) * tiles * LANES)
        y = dot(twice, both_ref[:, columns]) + dot(tl, both_ref[:SIDE, columns])
        for k in range(tiles):
            for r in range(rows_of):
                where = pl.ds(i * span + k * rows_of + r, groups, stride=room)
                out_ref[where, :] = y[r * groups : (r + 1) * groups, k * LANES : (k + 1) * LANES]
        store(i).start()
    for i in range(CUTS):
        store(i).wait()


def local(gradients, momentum, weights):
    shape = gradients.shape
    new_momentum = rowwise(blend_kernel, "blend", None, flat(momentum), flat(gradients))
    axes = ("rows", "cols")
    x = lax.all_to_all(new_momentum, axes, split_axis=0, concat_axis=0, tiled=True)
    room = x.shape[0] + PAD * SIDE // shape[1]
    y = pl.pallas_call(
        functools.partial(orthogonal, shape[1]),
        out_shape=jax.ShapeDtypeStruct(x.shape, x.dtype),
        in_specs=[pl.BlockSpec(memory_space=pl.ANY)],
        out_specs=pl.BlockSpec(memory_space=pl.ANY),
        scratch_shapes=[
            pltpu.VMEM((room, LANES), jnp.float32),
            pltpu.VMEM((room, LANES), jnp.float32),
            pltpu.VMEM((2 * SIDE, x.size // SIDE), jnp.bfloat16),
            pltpu.SemaphoreType.DMA((CUTS,)),
            pltpu.SemaphoreType.DMA((CUTS,)),
        ],
        name="orthogonal",
    )(x)
    y = lax.all_to_all(y, axes, split_axis=0, concat_axis=0, tiled=True)
    new_weights = rowwise(decay_kernel, "decay", LIMIT, flat(weights), y)
    return (unflat(new_weights, shape), unflat(new_momentum, shape))


def solution(mesh):
    placed = P(None, "rows", "cols")
    return jax.shard_map(
        local,
        mesh=mesh,
        in_specs=(placed, placed, placed),
        out_specs=(placed, placed),
        check_vma=False,
    )
```

```python
import functools

import jax
import jax.numpy as jnp
from jax import lax
from jax.experimental import pallas as pl
from jax.experimental.layout import Layout, with_layout_constraint
from jax.experimental.pallas import tpu as pltpu
from jax.sharding import PartitionSpec as P

ITERS = 4

hold_rate = 0.8
learn_rate = 0.8
decay_rate = 0.1

LANES = 128
SIDE = 128
CUTS = 4
PAD = 8
LIMIT = 24 << 20


def tiled(x):
    return with_layout_constraint(x, Layout(major_to_minor=(0, 2, 1, 3)))


def flat(x):
    mats, rows, wide = x.shape
    x = tiled(x.reshape(mats, rows, wide // LANES, LANES))
    return x.transpose(0, 2, 1, 3).reshape(-1, LANES)


def unflat(x, shape):
    mats, rows, wide = shape
    x = x.reshape(mats, wide // LANES, rows, LANES).transpose(0, 2, 1, 3)
    return tiled(x).reshape(shape)


def split(x):
    high = x.astype(jnp.bfloat16)
    return high, (x - high.astype(jnp.float32)).astype(jnp.bfloat16)


def dot(a, b, dims=((1,), (0,))):
    return lax.dot_general(a, b, (dims, ((), ())), preferred_element_type=jnp.float32)


def dot3(a, b):
    ah, al = split(a)
    bh, bl = split(b)
    return dot(ah, bh) + (dot(ah, bl) + dot(al, bh))


def blend_kernel(momentum_ref, gradients_ref, out_ref, a_ref, b_ref, c_ref, a_sem, b_sem, c_sem):
    cut = out_ref.shape[0] // CUTS
    copies = []
    for i in range(CUTS):
        at = pl.ds(i * cut, cut)
        copies.append(
            (
                pltpu.make_async_copy(momentum_ref.at[at], a_ref.at[at], a_sem.at[i]),
                pltpu.make_async_copy(gradients_ref.at[at], b_ref.at[at], b_sem.at[i]),
                pltpu.make_async_copy(c_ref.at[at], out_ref.at[at], c_sem.at[i]),
            )
        )
        copies[i][0].start()
        copies[i][1].start()
    for i in range(CUTS):
        copies[i][0].wait()
        copies[i][1].wait()
        at = pl.ds(i * cut, cut)
        c_ref[at] = hold_rate * a_ref[at] + b_ref[at]
        copies[i][2].start()
    for i in range(CUTS):
        copies[i][2].wait()


def blend(momentum, gradients):
    return pl.pallas_call(
        blend_kernel,
        out_shape=jax.ShapeDtypeStruct(momentum.shape, momentum.dtype),
        in_specs=[pl.BlockSpec(memory_space=pl.ANY)] * 2,
        out_specs=pl.BlockSpec(memory_space=pl.ANY),
        scratch_shapes=[pltpu.VMEM(momentum.shape, momentum.dtype)] * 3
        + [pltpu.SemaphoreType.DMA((CUTS,))] * 3,
        name="blend",
    )(momentum, gradients)


def decay_kernel(weights_ref, step_ref, out_ref, held_ref, sem):
    cut = out_ref.shape[0] // CUTS
    copies = []
    for i in range(CUTS):
        at = pl.ds(i * cut, cut)
        held_ref[at] = (1.0 - learn_rate * decay_rate) * weights_ref[at] - step_ref[at]
        copies.append(pltpu.make_async_copy(held_ref.at[at], out_ref.at[at], sem.at[i]))
        copies[i].start()
    for copy in copies:
        copy.wait()


def decay(weights, step):
    return pl.pallas_call(
        decay_kernel,
        out_shape=jax.ShapeDtypeStruct(weights.shape, weights.dtype),
        in_specs=[pl.BlockSpec(memory_space=pltpu.VMEM)] * 2,
        out_specs=pl.BlockSpec(memory_space=pltpu.HBM),
        scratch_shapes=[pltpu.VMEM(weights.shape, weights.dtype), pltpu.SemaphoreType.DMA((CUTS,))],
        compiler_params=pltpu.CompilerParams(vmem_limit_bytes=LIMIT),
        name="decay",
    )(weights, step)


def orthogonal(rows_of, x_ref, y_ref, in_ref, out_ref, both_ref, in_sem, out_sem):
    groups = SIDE // rows_of
    step = x_ref.shape[0] // groups
    room = step + PAD
    span = step // CUTS
    tiles = span // rows_of

    def cut(ref, rows, i):
        return ref.reshape(groups, rows, LANES).at[:, pl.ds(i * span, span), :]

    def fetch(i):
        return pltpu.make_async_copy(cut(x_ref, step, i), cut(in_ref, room, i), in_sem.at[i])

    def store(i):
        return pltpu.make_async_copy(cut(out_ref, room, i), cut(y_ref, step, i), out_sem.at[i])

    for i in range(CUTS):
        fetch(i).start()
    grams = jnp.zeros((SIDE, 2 * SIDE), jnp.float32)
    for i in range(CUTS):
        fetch(i).wait()
        for k in range(tiles):
            for r in range(rows_of):
                high, low = split(in_ref[pl.ds(i * span + k * rows_of + r, groups, stride=room), :])
                columns = slice((i * tiles + k) * LANES, (i * tiles + k + 1) * LANES)
                both_ref[r * groups : (r + 1) * groups, columns] = high
                both_ref[SIDE + r * groups : SIDE + (r + 1) * groups, columns] = low
        columns = slice(i * tiles * LANES, (i + 1) * tiles * LANES)
        grams += dot(both_ref[:SIDE, columns], both_ref[:, columns], ((1,), (1,)))
    cross = grams[:, SIDE:]
    gram = grams[:, :SIDE] + (cross + cross.T)
    one = (
        lax.broadcasted_iota(jnp.int32, (SIDE, SIDE), 0)
        == lax.broadcasted_iota(jnp.int32, (SIDE, SIDE), 1)
    ).astype(jnp.float32)
    scale = lax.rsqrt(jnp.sum(gram * one, axis=(0, 1), keepdims=True) + 1e-06)
    gram = gram * scale * scale
    total = None
    for turn in range(ITERS):
        mixed = 3.4445 * one - 4.775 * gram + 2.0315 * dot3(gram, gram)
        total = mixed if total is None else dot3(mixed, total)
        if turn < ITERS - 1:
            gram = dot3(mixed, dot3(mixed, gram))
    th, tl = split(total * (learn_rate * scale))
    twice = jnp.concatenate([th, th], axis=1)
    for i in range(CUTS):
        columns = slice(i * tiles * LANES, (i + 1) * tiles * LANES)
        y = dot(twice, both_ref[:, columns]) + dot(tl, both_ref[:SIDE, columns])
        for k in range(tiles):
            for r in range(rows_of):
                where = pl.ds(i * span + k * rows_of + r, groups, stride=room)
                out_ref[where, :] = y[r * groups : (r + 1) * groups, k * LANES : (k + 1) * LANES]
        store(i).start()
    for i in range(CUTS):
        store(i).wait()


def local(gradients, momentum, weights):
    shape = gradients.shape
    new_momentum = blend(flat(momentum), flat(gradients))
    axes = ("rows", "cols")
    x = lax.all_to_all(new_momentum, axes, split_axis=0, concat_axis=0, tiled=True)
    room = x.shape[0] + PAD * SIDE // shape[1]
    y = pl.pallas_call(
        functools.partial(orthogonal, shape[1]),
        out_shape=jax.ShapeDtypeStruct(x.shape, x.dtype),
        in_specs=[pl.BlockSpec(memory_space=pl.ANY)],
        out_specs=pl.BlockSpec(memory_space=pl.ANY),
        scratch_shapes=[
            pltpu.VMEM((room, LANES), jnp.float32),
            pltpu.VMEM((room, LANES), jnp.float32),
            pltpu.VMEM((2 * SIDE, x.size // SIDE), jnp.bfloat16),
            pltpu.SemaphoreType.DMA((CUTS,)),
            pltpu.SemaphoreType.DMA((CUTS,)),
        ],
        name="orthogonal",
    )(x)
    y = lax.all_to_all(y, axes, split_axis=0, concat_axis=0, tiled=True)
    new_weights = decay(flat(weights), y)
    return (unflat(new_weights, shape), unflat(new_momentum, shape))


def solution(mesh):
    placed = P(None, "rows", "cols")
    return jax.shard_map(
        local,
        mesh=mesh,
        in_specs=(placed, placed, placed),
        out_specs=(placed, placed),
        check_vma=False,
    )
```

```python
import functools

import jax
import jax.numpy as jnp
from jax import lax
from jax.experimental import pallas as pl
from jax.experimental.layout import Layout, with_layout_constraint
from jax.experimental.pallas import tpu as pltpu
from jax.sharding import PartitionSpec as P

ITERS = 4

hold_rate = 0.8
learn_rate = 0.8
decay_rate = 0.1

LANES = 128
SIDE = 128
CUTS = 4
LIMIT = 24 << 20


def tiled(x):
    return with_layout_constraint(x, Layout(major_to_minor=(0, 2, 1, 3)))


def flat(x):
    mats, rows, wide = x.shape
    x = tiled(x.reshape(mats, rows, wide // LANES, LANES))
    return x.transpose(0, 2, 1, 3).reshape(-1, LANES)


def unflat(x, shape):
    mats, rows, wide = shape
    x = x.reshape(mats, wide // LANES, rows, LANES).transpose(0, 2, 1, 3)
    return tiled(x).reshape(shape)


def split(x):
    high = x.astype(jnp.bfloat16)
    return high, (x - high.astype(jnp.float32)).astype(jnp.bfloat16)


def dot(a, b, dims=((1,), (0,))):
    return lax.dot_general(a, b, (dims, ((), ())), preferred_element_type=jnp.float32)


def dot3(a, b):
    ah, al = split(a)
    bh, bl = split(b)
    return dot(ah, bh) + (dot(ah, bl) + dot(al, bh))


def blend_kernel(momentum_ref, gradients_ref, out_ref, a_ref, b_ref, c_ref, a_sem, b_sem, c_sem):
    cut = out_ref.shape[0] // CUTS
    copies = []
    for i in range(CUTS):
        at = pl.ds(i * cut, cut)
        copies.append(
            (
                pltpu.make_async_copy(momentum_ref.at[at], a_ref.at[at], a_sem.at[i]),
                pltpu.make_async_copy(gradients_ref.at[at], b_ref.at[at], b_sem.at[i]),
                pltpu.make_async_copy(c_ref.at[at], out_ref.at[at], c_sem.at[i]),
            )
        )
        copies[i][0].start()
        copies[i][1].start()
    for i in range(CUTS):
        copies[i][0].wait()
        copies[i][1].wait()
        at = pl.ds(i * cut, cut)
        c_ref[at] = hold_rate * a_ref[at] + b_ref[at]
        copies[i][2].start()
    for i in range(CUTS):
        copies[i][2].wait()


def blend(momentum, gradients):
    return pl.pallas_call(
        blend_kernel,
        out_shape=jax.ShapeDtypeStruct(momentum.shape, momentum.dtype),
        in_specs=[pl.BlockSpec(memory_space=pl.ANY)] * 2,
        out_specs=pl.BlockSpec(memory_space=pl.ANY),
        scratch_shapes=[pltpu.VMEM(momentum.shape, momentum.dtype)] * 3
        + [pltpu.SemaphoreType.DMA((CUTS,))] * 3,
        name="blend",
    )(momentum, gradients)


def decay_kernel(weights_ref, step_ref, out_ref, held_ref, sem):
    cut = out_ref.shape[0] // CUTS
    copies = []
    for i in range(CUTS):
        at = pl.ds(i * cut, cut)
        held_ref[at] = (1.0 - learn_rate * decay_rate) * weights_ref[at] - step_ref[at]
        copies.append(pltpu.make_async_copy(held_ref.at[at], out_ref.at[at], sem.at[i]))
        copies[i].start()
    for copy in copies:
        copy.wait()


def decay(weights, step):
    return pl.pallas_call(
        decay_kernel,
        out_shape=jax.ShapeDtypeStruct(weights.shape, weights.dtype),
        in_specs=[pl.BlockSpec(memory_space=pltpu.VMEM)] * 2,
        out_specs=pl.BlockSpec(memory_space=pltpu.HBM),
        scratch_shapes=[pltpu.VMEM(weights.shape, weights.dtype), pltpu.SemaphoreType.DMA((CUTS,))],
        compiler_params=pltpu.CompilerParams(vmem_limit_bytes=LIMIT),
        name="decay",
    )(weights, step)


def orthogonal(rows_of, wide_of, x_ref, y_ref, both_ref):
    groups = SIDE // rows_of
    step = wide_of // LANES * rows_of
    tiles = wide_of // LANES
    chunks = x_ref.shape[0] // (groups * step)

    def where(i, k, r):
        return pl.ds(i * groups * step + k * rows_of + r, groups, stride=step)

    grams = jnp.zeros((SIDE, 2 * SIDE), jnp.float32)
    for i in range(chunks):
        for k in range(tiles):
            for r in range(rows_of):
                high, low = split(x_ref[where(i, k, r), :])
                columns = slice((i * tiles + k) * LANES, (i * tiles + k + 1) * LANES)
                both_ref[r * groups : (r + 1) * groups, columns] = high
                both_ref[SIDE + r * groups : SIDE + (r + 1) * groups, columns] = low
        columns = slice(i * tiles * LANES, (i + 1) * tiles * LANES)
        grams += dot(both_ref[:SIDE, columns], both_ref[:, columns], ((1,), (1,)))
    cross = grams[:, SIDE:]
    gram = grams[:, :SIDE] + (cross + cross.T)
    one = (
        lax.broadcasted_iota(jnp.int32, (SIDE, SIDE), 0)
        == lax.broadcasted_iota(jnp.int32, (SIDE, SIDE), 1)
    ).astype(jnp.float32)
    scale = lax.rsqrt(jnp.sum(gram * one, axis=(0, 1), keepdims=True) + 1e-06)
    gram = gram * scale * scale
    total = None
    for turn in range(ITERS):
        mixed = 3.4445 * one - 4.775 * gram + 2.0315 * dot3(gram, gram)
        total = mixed if total is None else dot3(mixed, total)
        if turn < ITERS - 1:
            gram = dot3(mixed, dot3(mixed, gram))
    th, tl = split(total * (learn_rate * scale))
    twice = jnp.concatenate([th, th], axis=1)
    for i in range(chunks):
        columns = slice(i * tiles * LANES, (i + 1) * tiles * LANES)
        y = dot(twice, both_ref[:, columns]) + dot(tl, both_ref[:SIDE, columns])
        for k in range(tiles):
            for r in range(rows_of):
                y_ref[where(i, k, r), :] = y[r * groups : (r + 1) * groups, k * LANES : (k + 1) * LANES]


def local(gradients, momentum, weights):
    shape = gradients.shape
    new_momentum = blend(flat(momentum), flat(gradients))
    axes = ("cols", "rows")
    x = lax.all_to_all(new_momentum, axes, split_axis=0, concat_axis=0, tiled=True)
    y = pl.pallas_call(
        functools.partial(orthogonal, shape[1], shape[2]),
        out_shape=jax.ShapeDtypeStruct(x.shape, x.dtype),
        in_specs=[pl.BlockSpec(memory_space=pltpu.VMEM)],
        out_specs=pl.BlockSpec(memory_space=pltpu.VMEM),
        scratch_shapes=[pltpu.VMEM((2 * SIDE, x.size // SIDE), jnp.bfloat16)],
        compiler_params=pltpu.CompilerParams(vmem_limit_bytes=LIMIT),
        name="orthogonal",
    )(x)
    y = lax.all_to_all(y, axes, split_axis=0, concat_axis=0, tiled=True)
    new_weights = decay(flat(weights), y)
    return (unflat(new_weights, shape), unflat(new_momentum, shape))


def solution(mesh):
    placed = P(None, "rows", "cols")
    return jax.shard_map(
        local,
        mesh=mesh,
        in_specs=(placed, placed, placed),
        out_specs=(placed, placed),
        check_vma=False,
    )
```

```python
import functools

import jax
import jax.numpy as jnp
from jax import lax
from jax.experimental import pallas as pl
from jax.experimental.layout import Layout, with_layout_constraint
from jax.experimental.pallas import tpu as pltpu
from jax.sharding import PartitionSpec as P

ITERS = 4

hold_rate = 0.8
learn_rate = 0.8
decay_rate = 0.1

LANES = 128
SIDE = 128
CUTS = 4
PACK = 16
LIMIT = 24 << 20


def tiled(x):
    return with_layout_constraint(x, Layout(major_to_minor=(0, 2, 1, 3)))


def flat(x):
    mats, rows, wide = x.shape
    x = tiled(x.reshape(mats, rows, wide // LANES, LANES))
    return x.transpose(0, 2, 1, 3).reshape(-1, LANES)


def unflat(x, shape):
    mats, rows, wide = shape
    x = x.reshape(mats, wide // LANES, rows, LANES).transpose(0, 2, 1, 3)
    return tiled(x).reshape(shape)


def split(x):
    high = x.astype(jnp.bfloat16)
    return high, (x - high.astype(jnp.float32)).astype(jnp.bfloat16)


def dot(a, b, dims=((1,), (0,))):
    return lax.dot_general(a, b, (dims, ((), ())), preferred_element_type=jnp.float32)


def dot3(a, b):
    ah, al = split(a)
    bh, bl = split(b)
    return dot(ah, bh) + (dot(ah, bl) + dot(al, bh))


def blend_kernel(momentum_ref, gradients_ref, out_ref, a_ref, b_ref, c_ref, a_sem, b_sem, c_sem):
    cut = out_ref.shape[0] // CUTS
    copies = []
    for i in range(CUTS):
        at = pl.ds(i * cut, cut)
        copies.append(
            (
                pltpu.make_async_copy(momentum_ref.at[at], a_ref.at[at], a_sem.at[i]),
                pltpu.make_async_copy(gradients_ref.at[at], b_ref.at[at], b_sem.at[i]),
                pltpu.make_async_copy(c_ref.at[at], out_ref.at[at], c_sem.at[i]),
            )
        )
        copies[i][0].start()
        copies[i][1].start()
    for i in range(CUTS):
        copies[i][0].wait()
        copies[i][1].wait()
        at = pl.ds(i * cut, cut)
        c_ref[at] = hold_rate * a_ref[at] + b_ref[at]
        copies[i][2].start()
    for i in range(CUTS):
        copies[i][2].wait()


def blend(momentum, gradients):
    return pl.pallas_call(
        blend_kernel,
        out_shape=jax.ShapeDtypeStruct(momentum.shape, momentum.dtype),
        in_specs=[pl.BlockSpec(memory_space=pl.ANY)] * 2,
        out_specs=pl.BlockSpec(memory_space=pl.ANY),
        scratch_shapes=[pltpu.VMEM(momentum.shape, momentum.dtype)] * 3
        + [pltpu.SemaphoreType.DMA((CUTS,))] * 3,
        name="blend",
    )(momentum, gradients)


def decay_kernel(weights_ref, step_ref, out_ref, held_ref, sem):
    cut = out_ref.shape[0] // CUTS
    copies = []
    for i in range(CUTS):
        at = pl.ds(i * cut, cut)
        held_ref[at] = (1.0 - learn_rate * decay_rate) * weights_ref[at] - step_ref[at]
        copies.append(pltpu.make_async_copy(held_ref.at[at], out_ref.at[at], sem.at[i]))
        copies[i].start()
    for copy in copies:
        copy.wait()


def decay(weights, step):
    return pl.pallas_call(
        decay_kernel,
        out_shape=jax.ShapeDtypeStruct(weights.shape, weights.dtype),
        in_specs=[pl.BlockSpec(memory_space=pltpu.VMEM)] * 2,
        out_specs=pl.BlockSpec(memory_space=pltpu.HBM),
        scratch_shapes=[pltpu.VMEM(weights.shape, weights.dtype), pltpu.SemaphoreType.DMA((CUTS,))],
        compiler_params=pltpu.CompilerParams(vmem_limit_bytes=LIMIT),
        name="decay",
    )(weights, step)


def orthogonal(rows_of, wide_of, x_ref, y_ref, both_ref):
    groups = SIDE // rows_of
    step = wide_of // LANES * rows_of
    tiles = wide_of // LANES
    chunks = x_ref.shape[0] // (groups * step)

    gram = jnp.zeros((SIDE, SIDE), jnp.float32)
    cross = jnp.zeros((SIDE, SIDE), jnp.float32)
    for i in range(chunks):
        for g in range(0, groups, PACK):
            block = x_ref[pl.ds((i * groups + g) * step, PACK * step), :].reshape(PACK, step, LANES)
            block = jnp.transpose(block, (1, 0, 2))
            for k in range(tiles):
                columns = slice((i * tiles + k) * LANES, (i * tiles + k + 1) * LANES)
                for r in range(rows_of):
                    high, low = split(block[k * rows_of + r])
                    row = r * groups + g
                    both_ref[row : row + PACK, columns] = high
                    both_ref[SIDE + row : SIDE + row + PACK, columns] = low
        columns = slice(i * tiles * LANES, (i + 1) * tiles * LANES)
        gram += dot(both_ref[:SIDE, columns], both_ref[:SIDE, columns], ((1,), (1,)))
        cross += dot(both_ref[:SIDE, columns], both_ref[SIDE:, columns], ((1,), (1,)))
    gram += cross + cross.T
    one = (
        lax.broadcasted_iota(jnp.int32, (SIDE, SIDE), 0)
        == lax.broadcasted_iota(jnp.int32, (SIDE, SIDE), 1)
    ).astype(jnp.float32)
    scale = lax.rsqrt(jnp.sum(gram * one, axis=(0, 1), keepdims=True) + 1e-06)
    gram = gram * scale * scale
    total = None
    for turn in range(ITERS):
        mixed = 3.4445 * one - 4.775 * gram + 2.0315 * dot3(gram, gram)
        total = mixed if total is None else dot3(mixed, total)
        if turn < ITERS - 1:
            gram = dot3(mixed, dot3(mixed, gram))
    th, tl = split(total * (learn_rate * scale))
    twice = jnp.concatenate(
        [jnp.concatenate([th, th], axis=1), jnp.concatenate([tl, jnp.zeros_like(tl)], axis=1)], axis=0
    )
    for i in range(chunks):
        columns = slice(i * tiles * LANES, (i + 1) * tiles * LANES)
        y = dot(twice, both_ref[:, columns])
        y = y[:SIDE] + y[SIDE:]
        for g in range(0, groups, PACK):
            block = jnp.stack(
                [
                    y[r * groups + g : r * groups + g + PACK, k * LANES : (k + 1) * LANES]
                    for k in range(tiles)
                    for r in range(rows_of)
                ]
            )
            block = jnp.transpose(block, (1, 0, 2)).reshape(PACK * step, LANES)
            y_ref[pl.ds((i * groups + g) * step, PACK * step), :] = block


def local(gradients, momentum, weights):
    shape = gradients.shape
    new_momentum = blend(flat(momentum), flat(gradients))
    axes = ("cols", "rows")
    x = lax.all_to_all(new_momentum, axes, split_axis=0, concat_axis=0, tiled=True)
    y = pl.pallas_call(
        functools.partial(orthogonal, shape[1], shape[2]),
        out_shape=jax.ShapeDtypeStruct(x.shape, x.dtype),
        in_specs=[pl.BlockSpec(memory_space=pltpu.VMEM)],
        out_specs=pl.BlockSpec(memory_space=pltpu.VMEM),
        scratch_shapes=[pltpu.VMEM((2 * SIDE, x.size // SIDE), jnp.bfloat16)],
        compiler_params=pltpu.CompilerParams(vmem_limit_bytes=LIMIT),
        name="orthogonal",
    )(x)
    y = lax.all_to_all(y, axes, split_axis=0, concat_axis=0, tiled=True)
    new_weights = decay(flat(weights), y)
    return (unflat(new_weights, shape), unflat(new_momentum, shape))


def solution(mesh):
    placed = P(None, "rows", "cols")
    return jax.shard_map(
        local,
        mesh=mesh,
        in_specs=(placed, placed, placed),
        out_specs=(placed, placed),
        check_vma=False,
    )
```

```python
import functools

import jax
import jax.numpy as jnp
from jax import lax
from jax.experimental import pallas as pl
from jax.experimental.layout import Layout, with_layout_constraint
from jax.experimental.pallas import tpu as pltpu
from jax.sharding import PartitionSpec as P

ITERS = 4

hold_rate = 0.8
learn_rate = 0.8
decay_rate = 0.1

LANES = 128
SIDE = 128
CUTS = 8
PACK = 16
LIMIT = 24 << 20


def tiled(x):
    return with_layout_constraint(x, Layout(major_to_minor=(0, 2, 1, 3)))


def flat(x):
    mats, rows, wide = x.shape
    x = tiled(x.reshape(mats, rows, wide // LANES, LANES))
    return x.transpose(0, 2, 1, 3).reshape(-1, LANES)


def unflat(x, shape):
    mats, rows, wide = shape
    x = x.reshape(mats, wide // LANES, rows, LANES).transpose(0, 2, 1, 3)
    return tiled(x).reshape(shape)


def split(x):
    high = x.astype(jnp.bfloat16)
    return high, (x - high.astype(jnp.float32)).astype(jnp.bfloat16)


def dot(a, b, dims=((1,), (0,))):
    return lax.dot_general(a, b, (dims, ((), ())), preferred_element_type=jnp.float32)


def dot3(a, b):
    ah, al = split(a)
    bh, bl = split(b)
    return dot(ah, bh) + (dot(ah, bl) + dot(al, bh))


def blend_kernel(momentum_ref, gradients_ref, out_ref, a_ref, b_ref, c_ref, a_sem, b_sem, c_sem):
    cut = out_ref.shape[0] // CUTS
    copies = []
    for i in range(CUTS):
        at = pl.ds(i * cut, cut)
        copies.append(
            (
                pltpu.make_async_copy(momentum_ref.at[at], a_ref.at[at], a_sem.at[i]),
                pltpu.make_async_copy(gradients_ref.at[at], b_ref.at[at], b_sem.at[i]),
                pltpu.make_async_copy(c_ref.at[at], out_ref.at[at], c_sem.at[i]),
            )
        )
        copies[i][0].start()
        copies[i][1].start()
    for i in range(CUTS):
        copies[i][0].wait()
        copies[i][1].wait()
        at = pl.ds(i * cut, cut)
        c_ref[at] = hold_rate * a_ref[at] + b_ref[at]
        copies[i][2].start()
    for i in range(CUTS):
        copies[i][2].wait()


def blend(momentum, gradients):
    return pl.pallas_call(
        blend_kernel,
        out_shape=jax.ShapeDtypeStruct(momentum.shape, momentum.dtype),
        in_specs=[pl.BlockSpec(memory_space=pl.ANY)] * 2,
        out_specs=pl.BlockSpec(memory_space=pl.ANY),
        scratch_shapes=[pltpu.VMEM(momentum.shape, momentum.dtype)] * 3
        + [pltpu.SemaphoreType.DMA((CUTS,))] * 3,
        name="blend",
    )(momentum, gradients)


def decay_kernel(weights_ref, step_ref, out_ref, held_ref, sem):
    cut = out_ref.shape[0] // CUTS
    copies = []
    for i in range(CUTS):
        at = pl.ds(i * cut, cut)
        held_ref[at] = (1.0 - learn_rate * decay_rate) * weights_ref[at] - step_ref[at]
        copies.append(pltpu.make_async_copy(held_ref.at[at], out_ref.at[at], sem.at[i]))
        copies[i].start()
    for copy in copies:
        copy.wait()


def decay(weights, step):
    return pl.pallas_call(
        decay_kernel,
        out_shape=jax.ShapeDtypeStruct(weights.shape, weights.dtype),
        in_specs=[pl.BlockSpec(memory_space=pltpu.VMEM)] * 2,
        out_specs=pl.BlockSpec(memory_space=pltpu.HBM),
        scratch_shapes=[pltpu.VMEM(weights.shape, weights.dtype), pltpu.SemaphoreType.DMA((CUTS,))],
        compiler_params=pltpu.CompilerParams(vmem_limit_bytes=LIMIT),
        name="decay",
    )(weights, step)


def orthogonal(rows_of, wide_of, x_ref, y_ref, both_ref):
    groups = SIDE // rows_of
    step = wide_of // LANES * rows_of
    tiles = wide_of // LANES
    chunks = x_ref.shape[0] // (groups * step)

    gram = jnp.zeros((SIDE, SIDE), jnp.float32)
    cross = jnp.zeros((SIDE, SIDE), jnp.float32)
    for i in range(chunks):
        for g in range(0, groups, PACK):
            block = jnp.stack([x_ref[pl.ds(((g + p) * chunks + i) * step, step), :] for p in range(PACK)])
            block = jnp.transpose(block, (1, 0, 2))
            for k in range(tiles):
                columns = slice((i * tiles + k) * LANES, (i * tiles + k + 1) * LANES)
                for r in range(rows_of):
                    high, low = split(block[k * rows_of + r])
                    row = r * groups + g
                    both_ref[row : row + PACK, columns] = high
                    both_ref[SIDE + row : SIDE + row + PACK, columns] = low
        columns = slice(i * tiles * LANES, (i + 1) * tiles * LANES)
        gram += dot(both_ref[:SIDE, columns], both_ref[:SIDE, columns], ((1,), (1,)))
        cross += dot(both_ref[:SIDE, columns], both_ref[SIDE:, columns], ((1,), (1,)))
    gram += cross + cross.T
    one = (
        lax.broadcasted_iota(jnp.int32, (SIDE, SIDE), 0)
        == lax.broadcasted_iota(jnp.int32, (SIDE, SIDE), 1)
    ).astype(jnp.float32)
    scale = lax.rsqrt(jnp.sum(gram * one, axis=(0, 1), keepdims=True) + 1e-06)
    gram = gram * scale * scale
    total = None
    for turn in range(ITERS):
        mixed = 3.4445 * one - 4.775 * gram + 2.0315 * dot3(gram, gram)
        total = mixed if total is None else dot3(mixed, total)
        if turn < ITERS - 1:
            gram = dot3(mixed, dot3(mixed, gram))
    th, tl = split(total * (learn_rate * scale))
    twice = jnp.concatenate(
        [jnp.concatenate([th, th], axis=1), jnp.concatenate([tl, jnp.zeros_like(tl)], axis=1)], axis=0
    )
    for i in range(chunks):
        columns = slice(i * tiles * LANES, (i + 1) * tiles * LANES)
        y = dot(twice, both_ref[:, columns])
        y = y[:SIDE] + y[SIDE:]
        for g in range(0, groups, PACK):
            block = jnp.stack(
                [
                    y[r * groups + g : r * groups + g + PACK, k * LANES : (k + 1) * LANES]
                    for k in range(tiles)
                    for r in range(rows_of)
                ]
            )
            block = jnp.transpose(block, (1, 0, 2))
            for p in range(PACK):
                y_ref[pl.ds(((g + p) * chunks + i) * step, step), :] = block[p]


def local(gradients, momentum, weights):
    shape = gradients.shape
    new_momentum = blend(flat(momentum), flat(gradients))
    axes = ("rows", "cols")
    x = lax.all_to_all(new_momentum, axes, split_axis=0, concat_axis=0, tiled=True)
    y = pl.pallas_call(
        functools.partial(orthogonal, shape[1], shape[2]),
        out_shape=jax.ShapeDtypeStruct(x.shape, x.dtype),
        in_specs=[pl.BlockSpec(memory_space=pltpu.VMEM)],
        out_specs=pl.BlockSpec(memory_space=pltpu.VMEM),
        scratch_shapes=[pltpu.VMEM((2 * SIDE, x.size // SIDE), jnp.bfloat16)],
        compiler_params=pltpu.CompilerParams(vmem_limit_bytes=LIMIT),
        name="orthogonal",
    )(x)
    y = lax.all_to_all(y, axes, split_axis=0, concat_axis=0, tiled=True)
    new_weights = decay(flat(weights), y)
    return (unflat(new_weights, shape), unflat(new_momentum, shape))


def solution(mesh):
    placed = P(None, "rows", "cols")
    return jax.shard_map(
        local,
        mesh=mesh,
        in_specs=(placed, placed, placed),
        out_specs=(placed, placed),
        check_vma=False,
    )
```
